32 devices in a mesh: width: 8 (over z, core), lat: 4 (over y, x).
Axes of the slice: x: 2, y: 2, z: 4, core: 2. Of those that a mesh axis runs over, the one named last changes fastest.
Arguments:
- residuals: bfloat16 [384, 16384], P(None, 'width'), may hold values from -6 to 6
- encoder: bfloat16 [16384, 4096], P('width', 'lat'), may hold values from -0.046875 to 0.046875
- enc_bias: float32 [4096], P('lat'), may hold values from -3 to 3
- decoder: bfloat16 [4096, 16384], P('lat', 'width'), may hold values from -0.046875 to 0.046875
- dec_bias: float32 [16384], P('width'), may hold values from -3 to 3
Outputs:
- enc_grad: bfloat16 [16384, 4096], P('width', 'lat')
- new_decoder: bfloat16 [4096, 16384], P('lat', 'width')
The draws below stay inside these ranges and needn't reach their ends.
All inputs are finite; a program needn't handle non-finite values.
Results may differ from the reference program's by a relative error of at most 0.011.
Values may be sent and summed in bfloat16 or wider, within the bound.
A program may use at most 64 MiB of HBM per device.

```python
import jax
import jax.numpy as jnp
from jax import lax

D = 16384
TOK = 384
LATENTS = 4096
N_LAT = 4


def level_of(rng, shape, shards, least, top_value):
    loudness, own = 1.0, jax.random.fold_in(rng, 6)
    for position, blocks in shards:
        draws = jnp.exp(jax.random.uniform(jax.random.fold_in(own, position), (blocks,), jnp.float32, least / len(shards), top_value / len(shards)))
        loudness = loudness * jnp.repeat(draws, shape[position] // blocks).reshape([-1 if axis == position else 1 for axis in range(len(shape))])
    return loudness


def scatter_about(rng, dims, scale, most, cuts=(), held_as=jnp.bfloat16):
    result = jax.random.normal(rng, dims, jnp.float32) * scale
    if len(cuts) > 0:
        result = level_of(rng, dims, cuts, -0.22, 0.18) * result
    return jnp.clip(result, min=-most, max=most).astype(held_as)


def setup_inputs(seed: int = 0) -> dict:
    key_list = jax.random.split(jax.random.key(seed), 6)
    residuals = scatter_about(key_list[0], (TOK, D), 1.0, 6.0, ((1, 8),))
    encoder = scatter_about(key_list[1], (D, LATENTS), D ** -0.5, 0.046875, ((0, 8), (1, 4)))
    enc_bias = scatter_about(key_list[2], (LATENTS,), 0.5, 3.0, ((0, 4),), jnp.float32)
    decoder = scatter_about(key_list[3], (LATENTS, D), D ** -0.5, 0.046875, ((0, 4), (1, 8)))
    dec_bias = scatter_about(key_list[4], (D,), 0.5, 3.0, ((0, 8),), jnp.float32)
    return dict(residuals=residuals, encoder=encoder, enc_bias=enc_bias, decoder=decoder, dec_bias=dec_bias)


EPS = 1e-06
STEP = 0.0003
PENALTY = 0.5

def reference(residuals, encoder, enc_bias, decoder, dec_bias):
    pre = jnp.dot(residuals, encoder, preferred_element_type=jnp.float32) + enc_bias
    acts = jnp.maximum(pre, 0.0).astype(jnp.bfloat16)
    recon = jnp.dot(acts, decoder, preferred_element_type=jnp.float32)
    error = (recon + dec_bias - residuals.astype(jnp.float32)).astype(jnp.bfloat16)
    dacts = lax.dot_general(error, decoder, (((1,), (1,)), ((), ())), preferred_element_type=jnp.float32) + PENALTY
    dpre = jnp.where(pre > 0.0, dacts, 0.0).astype(jnp.bfloat16)
    enc_grad = lax.dot_general(residuals, dpre, (((0,), (0,)), ((), ())), preferred_element_type=jnp.float32).astype(jnp.bfloat16)
    blocks = N_LAT
    width = acts.shape[1] // blocks
    act_blocks = acts.reshape(acts.shape[0], blocks, width).transpose(1, 0, 2)
    dec_blocks = decoder.reshape(blocks, width, decoder.shape[1])

    def renorm(pair):
        act_blk, dec_blk = pair
        grad = lax.dot_general(act_blk, error, (((0,), (0,)), ((), ())), preferred_element_type=jnp.float32)
        weight = dec_blk.astype(jnp.float32)
        ww = lax.optimization_barrier(jnp.sum(weight * weight, axis=1, keepdims=True))
        gw = lax.optimization_barrier(jnp.sum(grad * weight, axis=1, keepdims=True))
        coef = gw / (ww + EPS)
        moved = weight - STEP * (grad - coef * weight)
        squared = lax.optimization_barrier(jnp.sum(moved * moved, axis=1, keepdims=True))
        return (moved / jnp.sqrt(squared + EPS)).astype(jnp.bfloat16)
    new_decoder = lax.map(renorm, (act_blocks, dec_blocks)).reshape(decoder.shape)
    return (enc_grad, new_decoder)
```

```python
import functools

import jax
import jax.numpy as jnp
from jax import lax
from jax.experimental import pallas as pl
from jax.experimental.pallas import tpu as pltpu
from jax.sharding import PartitionSpec as P

EPS = 1e-06
STEP = 0.0003
PENALTY = 0.5
MESH = pl.DeviceIdType.MESH
F32, BF16 = jnp.float32, jnp.bfloat16
NT = (((1,), (1,)), ((), ()))


def step_kernel(
    Z, NL, NK, NN,
    res_h, enc_h, bias, dec_h, dbias,
    nd_o, dp_o, rt_o,
    res_v, enc_v, dec_v, stA, rxA, sA, rA, preS, acts, actsT, rt_v,
    rf, sB, rB, err, dacc, sD, rxD, sS, rD, dp, grad, sacc, stv, rst, ss, rs2, nd_v,
    in_sem, out_sem,
    a1s, a1r, a2s, a2r, a3s, a3r, a4s, a4r,
    bs, br, cs, cr,
    d1s, d1r, d2s, d2r, d3s, d3r, d4s, d4r,
    e1s, e1r, e2s, e2r,
):
    T, DW = res_v.shape
    KB = acts.shape[-1]
    TB = acts.shape[-2]
    TL = err.shape[2]
    NB = err.shape[3]
    w = lax.axis_index("width")
    l = lax.axis_index("lat")
    z, c = w // 2, w % 2
    pc = 1 - c
    partner = (z * 2 + pc, l)

    def zdev(o):
        return ((z + o) % Z) * 2 + c, l

    def lat_to(o):
        return ((l // 2 + o // 2) % (NL // 2)) * 2 + (l % 2 + o % 2) % 2

    def lat_from(o):
        return ((l // 2 + NL // 2 - o // 2) % (NL // 2)) * 2 + (l % 2 + o % 2) % 2

    def rc(src, dst, ssem, rsem, dev):
        return pltpu.make_async_remote_copy(
            src_ref=src, dst_ref=dst, send_sem=ssem, recv_sem=rsem,
            device_id=dev, device_id_type=MESH,
        )

    def loop(n, f):
        lax.fori_loop(0, n, lambda i, _: (f(i), 0)[1], 0)

    c_res = pltpu.make_async_copy(res_h, res_v, in_sem.at[0])
    c_res.start()

    def enc_copy(k):
        return pltpu.make_async_copy(
            enc_h.at[:, pl.ds(pl.multiple_of(k * KB, KB), KB)], enc_v.at[k], in_sem.at[1 + k]
        )

    def dec_copy(n):
        return pltpu.make_async_copy(
            dec_h.at[:, pl.ds(pl.multiple_of(n * NB, NB), NB)], dec_v.at[n], in_sem.at[1 + NK + n]
        )

    for k in range(NK):
        enc_copy(k).start()
    for n in range(NN):
        dec_copy(n).start()

    barrier = pltpu.get_barrier_semaphore()
    pl.semaphore_signal(barrier, inc=1, device_id=partner, device_id_type=MESH)
    for o in range(1, Z):
        pl.semaphore_signal(barrier, inc=1, device_id=zdev(o), device_id_type=MESH)
    for o in range(1, NL):
        pl.semaphore_signal(barrier, inc=1, device_id=(w, lat_to(o)), device_id_type=MESH)

    def a1(k):
        return rc(stA.at[k, pc], rxA.at[k], a1s.at[k], a1r.at[k], partner)

    def a2(k, o):
        return rc(sA.at[k, (z + o) % Z], rA.at[k, o], a2s.at[k, o], a2r.at[k, o], zdev(o))

    def a3(k, o):
        return rc(acts.at[k, c, z], acts.at[k, c, z], a3s.at[k, o], a3r.at[k, o], zdev(o))

    def a3in(k, o):
        dst = acts.at[k, c, (z + Z - o) % Z]
        return rc(dst, dst, a3s.at[k, o], a3r.at[k, o], zdev(o))

    def a4(k):
        return rc(acts.at[k, c], acts.at[k, c], a4s.at[k], a4r.at[k], partner)

    def a4in(k):
        return rc(acts.at[k, pc], acts.at[k, pc], a4s.at[k], a4r.at[k], partner)

    def combine_a(k):
        a1(k).wait_recv()
        sA[k] = stA[k, c] + rxA[k]
        for o in range(1, Z):
            a2(k, o).start()

    c_res.wait()
    pl.semaphore_wait(barrier, 1 + (Z - 1) + (NL - 1))

    def pre_step(k):
        enc_copy(k).wait()
        p = jnp.dot(res_v[...], enc_v[k], preferred_element_type=F32)
        stA[k] = p.reshape(2, Z, TB, KB)
        a1(k).start()

        @pl.when(k > 0)
        def _():
            combine_a(k - 1)

    loop(NK, pre_step)
    combine_a(NK - 1)

    def fwd_a(k):
        for o in range(1, Z):
            a3in(k, o).wait_recv()
        a4(k).start()

    def act_step(k):
        for o in range(1, Z):
            a2(k, o).wait_recv()
        pre = sA[k, z]
        for o in range(1, Z):
            pre = pre + rA[k, o]
        pre = pre + bias[k]
        preS[k] = pre
        acts[k, c, z] = jnp.maximum(pre, 0.0).astype(BF16)
        for o in range(1, Z):
            a3(k, o).start()

        @pl.when(k > 0)
        def _():
            fwd_a(k - 1)

    RB = NB

    def rt_step(n):
        rt_v[n] = res_v[:, pl.ds(pl.multiple_of(n * RB, RB), RB)].T

    loop(NN, rt_step)
    rt_copy = pltpu.make_async_copy(rt_v, rt_o, out_sem.at[0])
    rt_copy.start()

    loop(NK, act_step)
    fwd_a(NK - 1)
    for n in range(NN):
        dec_copy(n).wait()
    loop(NK, lambda k: a4in(k).wait_recv())

    def b1(n, o):
        return rc(sB.at[n, lat_to(o)], rB.at[n, o], bs.at[n, o], br.at[n, o], (w, lat_to(o)))

    def c1(n, o):
        return rc(err.at[n, l], err.at[n, l], cs.at[n, o], cr.at[n, o], (w, lat_to(o)))

    def c1in(n, o):
        dst = err.at[n, lat_from(o)]
        return rc(dst, dst, cs.at[n, o], cr.at[n, o], (w, lat_to(o)))

    def rec_step(n):
        a = jnp.concatenate([acts[k].reshape(T, KB) for k in range(NK)], axis=1)
        r = jnp.dot(a, dec_v[n], preferred_element_type=F32).reshape(NL, TL, NB)
        rf[n] = r
        sB[n] = r.astype(BF16)
        for o in range(1, NL):
            b1(n, o).start()

    loop(NN, rec_step)

    def at_step(k):
        actsT[k] = acts[k].reshape(T, KB).T
        dacc[k] = jnp.zeros(dacc.shape[1:], F32)
        for s in range(3):
            sacc[s, k] = jnp.zeros(sacc.shape[2:], F32)

    loop(NK, at_step)

    def err_step(n):
        for o in range(1, NL):
            b1(n, o).wait_recv()
        r = rf[n, l]
        for o in range(1, NL):
            r = r + rB[n, o].astype(F32)
        own = res_v[
            pl.ds(pl.multiple_of(l * TL, TL), TL), pl.ds(pl.multiple_of(n * NB, NB), NB)
        ]
        err[n, l] = (r + dbias[n] - own.astype(F32)).astype(BF16)
        for o in range(1, NL):
            c1(n, o).start()

    loop(NN, err_step)

    def dacts_part(n, k):
        e = err[n].reshape(T, NB)
        d = lax.dot_general(
            e, dec_v[n, pl.ds(pl.multiple_of(k * KB, KB), KB), :], NT, preferred_element_type=F32
        )
        return dacc[k] + d.reshape(2, Z, TB, KB)

    def grad_part(n, k):
        g = jnp.dot(actsT[k], err[n].reshape(T, NB), preferred_element_type=F32)
        grad[n, k] = g
        wt = dec_v[n, pl.ds(pl.multiple_of(k * KB, KB), KB), :].astype(F32)
        for s, prod in enumerate((wt * wt, g * wt, g * g)):
            part = prod[:, 0:128]
            for j in range(1, NB // 128):
                part = part + prod[:, j * 128:(j + 1) * 128]
            sacc[s, k] += part

    def err_wait(n):
        for o in range(1, NL):
            c1in(n, o).wait_recv()

    def n_step(n):
        err_wait(n)

        def k_step(k):
            dacc[k] = dacts_part(n, k)
            grad_part(n, k)

        loop(NK, k_step)

    loop(NN - 1, n_step)

    def d1(k):
        return rc(sD.at[k, pc], rxD.at[k], d1s.at[k], d1r.at[k], partner)

    def d2(k, o):
        return rc(sS.at[k, (z + o) % Z], rD.at[k, o], d2s.at[k, o], d2r.at[k, o], zdev(o))

    def d3(k, o):
        return rc(dp.at[k, c, z], dp.at[k, c, z], d3s.at[k, o], d3r.at[k, o], zdev(o))

    def d3in(k, o):
        dst = dp.at[k, c, (z + Z - o) % Z]
        return rc(dst, dst, d3s.at[k, o], d3r.at[k, o], zdev(o))

    def d4(k):
        return rc(dp.at[k, c], dp.at[k, c], d4s.at[k], d4r.at[k], partner)

    def d4in(k):
        return rc(dp.at[k, pc], dp.at[k, pc], d4s.at[k], d4r.at[k], partner)

    def combine_d(k):
        d1(k).wait_recv()
        s = dacc[k, c] + rxD[k].astype(F32)
        dacc[k, c] = s
        sS[k] = s.astype(BF16)
        for o in range(1, Z):
            d2(k, o).start()

    last = NN - 1
    err_wait(last)

    def d_step(k):
        v = dacts_part(last, k)
        dacc[k] = v
        sD[k] = v.astype(BF16)
        d1(k).start()

        @pl.when(k > 0)
        def _():
            combine_d(k - 1)

    loop(NK, d_step)
    combine_d(NK - 1)

    def g_step(k):
        grad_part(last, k)
        for s in range(3):
            stv[k, s:s + 1, :] = jnp.sum(sacc[s, k].T, axis=0, keepdims=True)
        stv[k, 3:8, :] = jnp.zeros((5, KB), F32)

    def dp_step(k):
        for o in range(1, Z):
            d2(k, o).wait_recv()
        v = dacc[k, c, z]
        for o in range(1, Z):
            v = v + rD[k, o].astype(F32)
        dp[k, c, z] = jnp.where(preS[k] > 0.0, v + PENALTY, 0.0).astype(BF16)
        for o in range(1, Z):
            d3(k, o).start()

    def gd_step(k):
        g_step(k)
        dp_step(k)

    loop(NK, gd_step)

    e1 = rc(stv, rst, e1s, e1r, partner)
    e1.start()

    def e2(o):
        return rc(ss, rs2.at[o], e2s.at[o], e2r.at[o], zdev(o))

    e1.wait_recv()
    ss[...] = stv[...] + rst[...]
    for o in range(1, Z):
        e2(o).start()

    def fwd_d(k):
        for o in range(1, Z):
            d3in(k, o).wait_recv()
        d4(k).start()

    loop(NK, fwd_d)
    for o in range(1, Z):
        e2(o).wait_recv()

    def nd_copy(k):
        return pltpu.make_async_copy(
            nd_v.at[k], nd_o.at[pl.ds(pl.multiple_of(k * KB, KB), KB), :], out_sem.at[2 + k]
        )

    def nd_step(k):
        t = ss[k]
        for o in range(1, Z):
            t = t + rs2[o, k]
        ww, gw, gg = t[0:1], t[1:2], t[2:3]
        coef = gw / (ww + EPS)
        sq = (
            ww
            - 2.0 * STEP * (gw - coef * ww)
            + STEP * STEP * (gg - 2.0 * coef * gw + coef * coef * ww)
        )
        inv = 1.0 / jnp.sqrt(sq + EPS)
        up = jnp.broadcast_to((1.0 + STEP * coef) * inv, (128, KB)).T
        down = jnp.broadcast_to(STEP * inv, (128, KB)).T
        for n in range(NN):
            for j in range(NB // 128):
                wt = dec_v[n, pl.ds(pl.multiple_of(k * KB, KB), KB), j * 128:(j + 1) * 128]
                g = grad[n, k, :, j * 128:(j + 1) * 128]
                first = n * NB + j * 128
                nd_v[k, :, first:first + 128] = (wt.astype(F32) * up - g * down).astype(BF16)
        nd_copy(k).start()

    loop(NK, nd_step)
    loop(NK, lambda k: d4in(k).wait_recv())
    dp_copy = pltpu.make_async_copy(dp, dp_o, out_sem.at[1])
    dp_copy.start()

    def drain(k):
        for first in (a1, a4, d1, d4):
            first(k).wait_send()
        for o in range(1, Z):
            for each in (a2, a3, d2, d3):
                each(k, o).wait_send()
        nd_copy(k).wait()

    def drain_n(n):
        for o in range(1, NL):
            b1(n, o).wait_send()
            c1(n, o).wait_send()

    loop(NK, drain)
    loop(NN, drain_n)
    e1.wait_send()
    for o in range(1, Z):
        e2(o).wait_send()
    rt_copy.wait()
    dp_copy.wait()


def enc_grad_kernel(rt, dp, out):
    for k in range(dp.shape[0]):
        kb = dp.shape[2]
        out[:, k * kb:(k + 1) * kb] = jnp.dot(
            rt[0], dp[k], preferred_element_type=F32
        ).astype(BF16)


def fused(W, NL, residuals, encoder, enc_bias, decoder, dec_bias):
    T, DW = residuals.shape
    LL = encoder.shape[1]
    Z = W // 2
    NK, NN = 4, 4
    KB, NB = LL // NK, DW // NN
    TB, TL = T // W, T // NL
    V = pltpu.VMEM
    dma = pltpu.SemaphoreType.DMA
    scratch = [
        V((T, DW), BF16), V((NK, DW, KB), BF16), V((NN, LL, NB), BF16),
        V((NK, 2, Z, TB, KB), F32), V((NK, Z, TB, KB), F32), V((NK, Z, TB, KB), F32),
        V((NK, Z, TB, KB), F32), V((NK, TB, KB), F32),
        V((NK, 2, Z, TB, KB), BF16), V((NK, KB, T), BF16), V((NN, NB, T), BF16),
        V((NN, NL, TL, NB), F32), V((NN, NL, TL, NB), BF16), V((NN, NL, TL, NB), BF16),
        V((NN, NL, TL, NB), BF16),
        V((NK, 2, Z, TB, KB), F32), V((NK, 2, Z, TB, KB), BF16), V((NK, Z, TB, KB), BF16),
        V((NK, Z, TB, KB), BF16), V((NK, Z, TB, KB), BF16), V((NK, 2, Z, TB, KB), BF16),
        V((NN, NK, KB, NB), F32), V((3, NK, KB, 128), F32),
        V((NK, 8, KB), F32), V((NK, 8, KB), F32), V((NK, 8, KB), F32), V((Z, NK, 8, KB), F32),
        V((NK, KB, DW), BF16),
        dma((1 + NK + NN,)), dma((2 + NK,)),
        dma((NK,)), dma((NK,)), dma((NK, Z)), dma((NK, Z)), dma((NK, Z)), dma((NK, Z)),
        dma((NK,)), dma((NK,)),
        dma((NN, NL)), dma((NN, NL)), dma((NN, NL)), dma((NN, NL)),
        dma((NK,)), dma((NK,)), dma((NK, Z)), dma((NK, Z)), dma((NK, Z)), dma((NK, Z)),
        dma((NK,)), dma((NK,)),
        dma, dma, dma((Z,)), dma((Z,)),
    ]
    hbm = pl.BlockSpec(memory_space=pl.ANY)
    vm = pl.BlockSpec(memory_space=pltpu.VMEM)
    new_decoder, dp, rt = pl.pallas_call(
        functools.partial(step_kernel, Z, NL, NK, NN),
        out_shape=(
            jax.ShapeDtypeStruct((LL, DW), BF16),
            jax.ShapeDtypeStruct((NK, 2, Z, TB, KB), BF16),
            jax.ShapeDtypeStruct((NN, NB, T), BF16),
        ),
        in_specs=[hbm, hbm, vm, hbm, vm],
        out_specs=(hbm, hbm, hbm),
        scratch_shapes=scratch,
        compiler_params=pltpu.CompilerParams(
            collective_id=0, has_side_effects=True, vmem_limit_bytes=60 * 2**20
        ),
        name="sae_step",
    )(residuals, encoder, enc_bias.reshape(NK, 1, KB), decoder, dec_bias.reshape(NN, 1, NB))
    enc_grad = pl.pallas_call(
        enc_grad_kernel,
        grid=(NN,),
        out_shape=jax.ShapeDtypeStruct((DW, LL), BF16),
        in_specs=[
            pl.BlockSpec((1, NB, T), lambda i: (i, 0, 0)),
            pl.BlockSpec((NK, T, KB), lambda i: (0, 0, 0)),
        ],
        out_specs=pl.BlockSpec((NB, LL), lambda i: (i, 0)),
        compiler_params=pltpu.CompilerParams(vmem_limit_bytes=24 * 2**20),
        cost_estimate=pl.CostEstimate(
            flops=2 * T * DW * LL, bytes_accessed=2 * (T * DW + T * LL + DW * LL),
            transcendentals=0,
        ),
        name="enc_grad",
    )(rt, dp.reshape(NK, T, KB))
    return enc_grad, new_decoder


def plain(residuals, encoder, enc_bias, decoder, dec_bias):
    tokens = residuals.shape[0]
    lat_count = lax.axis_size("lat")
    lat_rows = tokens // lat_count
    rows = residuals
    pre_rows = (
        lax.psum_scatter(
            jnp.dot(rows, encoder, preferred_element_type=jnp.float32),
            "width",
            scatter_dimension=0,
            tiled=True,
        )
        + enc_bias
    )
    active_rows = pre_rows > 0.0
    act_rows = jnp.maximum(pre_rows, 0.0).astype(jnp.bfloat16)
    acts = lax.all_gather(act_rows, "width", axis=0, tiled=True)
    rows = acts
    recon_rows = lax.psum_scatter(
        jnp.dot(rows, decoder, preferred_element_type=jnp.float32),
        "lat",
        scatter_dimension=0,
        tiled=True,
    )
    first = lax.axis_index("lat") * lat_rows
    own_rows = lax.dynamic_slice_in_dim(residuals, first, lat_rows, 0)
    error_part = (recon_rows + dec_bias - own_rows.astype(jnp.float32)).astype(jnp.bfloat16)
    error = lax.all_gather(error_part, "lat", axis=0, tiled=True)
    rows = error
    dacts_rows = (
        lax.psum_scatter(
            lax.dot_general(
                rows, decoder, (((1,), (1,)), ((), ())), preferred_element_type=jnp.float32
            ),
            "width",
            scatter_dimension=0,
            tiled=True,
        )
        + PENALTY
    )
    dpre_part = jnp.where(active_rows, dacts_rows, 0.0).astype(jnp.bfloat16)
    dpre = lax.all_gather(dpre_part, "width", axis=0, tiled=True)
    enc_grad = lax.dot_general(
        residuals, dpre, (((0,), (0,)), ((), ())), preferred_element_type=jnp.float32
    ).astype(jnp.bfloat16)
    grad = lax.dot_general(
        acts, error, (((0,), (0,)), ((), ())), preferred_element_type=jnp.float32
    )
    weight = decoder.astype(jnp.float32)
    ww, gw, gg = lax.psum(
        (
            jnp.sum(weight * weight, axis=1),
            jnp.sum(grad * weight, axis=1),
            jnp.sum(grad * grad, axis=1),
        ),
        "width",
    )
    coef_row = gw / (ww + EPS)
    coef = coef_row[:, None]
    moved = weight - STEP * (grad - coef * weight)
    squared = (
        ww
        - 2.0 * STEP * (gw - coef_row * ww)
        + STEP * STEP * (gg - 2.0 * coef_row * gw + coef_row * coef_row * ww)
    )
    new_decoder = (moved / jnp.sqrt(squared + EPS)[:, None]).astype(jnp.bfloat16)
    return (enc_grad, new_decoder)


def per_device(W, NL, residuals, encoder, enc_bias, decoder, dec_bias):
    T, DW = residuals.shape
    LL = encoder.shape[1]
    args = (residuals, encoder, enc_bias, decoder, dec_bias)
    fits = W % 2 == 0 and NL % 2 == 0 and T % (16 * W) == 0 and T % (16 * NL) == 0
    if fits and DW % 512 == 0 and LL % 512 == 0 and T % 128 == 0:
        return fused(W, NL, *args)
    return plain(*args)


def solution(mesh):
    return jax.shard_map(
        functools.partial(per_device, mesh.shape["width"], mesh.shape["lat"]),
        mesh=mesh,
        in_specs=(P(None, "width"), P("width", "lat"), P("lat"), P("lat", "width"), P("width")),
        out_specs=(P("width", "lat"), P("lat", "width")),
        check_vma=False,
    )
```

```python
import functools

import jax
import jax.numpy as jnp
from jax import lax
from jax.experimental import pallas as pl
from jax.experimental.pallas import tpu as pltpu
from jax.sharding import PartitionSpec as P

EPS = 1e-06
STEP = 0.0003
PENALTY = 0.5
MESH = pl.DeviceIdType.MESH
F32, BF16 = jnp.float32, jnp.bfloat16
NT = (((1,), (1,)), ((), ()))


def step_kernel(
    Z, NL, NK, NN,
    res_h, enc_h, bias, dec_h, dbias,
    nd_o, dp_o, rt_o,
    res_v, enc_v, dec_v, stA, rxA, sA, rA, preS, acts, actsT, rt_v,
    rf, sB, rB, err, dacc, sD, rxD, sS, rD, dp, grad, sacc, stv, rst, ss, rs2, nd_v,
    in_sem, out_sem,
    a1s, a1r, a2s, a2r, a3s, a3r, a4s, a4r,
    bs, br, cs, cr,
    d1s, d1r, d2s, d2r, d3s, d3r, d4s, d4r,
    e1s, e1r, e2s, e2r,
):
    T, DW = res_v.shape
    H = acts.shape[0]
    TH = T // H
    TB, KC = acts.shape[-2:]
    KB = 2 * KC
    TL, NB = err.shape[-2:]
    w = lax.axis_index("width")
    l = lax.axis_index("lat")
    z, c = w // 2, w % 2
    pc = 1 - c
    partner = (z * 2 + pc, l)

    def zdev(o):
        return ((z + o) % Z) * 2 + c, l

    def lat_to(o):
        return ((l // 2 + o // 2) % (NL // 2)) * 2 + (l % 2 + o % 2) % 2

    def lat_from(o):
        return ((l // 2 + NL // 2 - o // 2) % (NL // 2)) * 2 + (l % 2 + o % 2) % 2

    def rc(src, dst, ssem, rsem, dev):
        return pltpu.make_async_remote_copy(
            src_ref=src, dst_ref=dst, send_sem=ssem, recv_sem=rsem,
            device_id=dev, device_id_type=MESH,
        )

    def loop(n, f):
        lax.fori_loop(0, n, lambda i, _: (f(i), 0)[1], 0)

    c_res = pltpu.make_async_copy(res_h, res_v, in_sem.at[0])
    c_res.start()

    def enc_copy(k):
        return pltpu.make_async_copy(
            enc_h.at[:, pl.ds(pl.multiple_of(k * KB, KB), KB)], enc_v.at[k], in_sem.at[1 + k]
        )

    def dec_copy(n):
        return pltpu.make_async_copy(
            dec_h.at[:, pl.ds(pl.multiple_of(n * NB, NB), NB)], dec_v.at[n], in_sem.at[1 + NK + n]
        )

    for k in range(NK):
        enc_copy(k).start()
    for n in range(NN):
        dec_copy(n).start()

    barrier = pltpu.get_barrier_semaphore()
    pl.semaphore_signal(barrier, inc=1, device_id=partner, device_id_type=MESH)
    for o in range(1, Z):
        pl.semaphore_signal(barrier, inc=1, device_id=zdev(o), device_id_type=MESH)
    for o in range(1, NL):
        pl.semaphore_signal(barrier, inc=1, device_id=(w, lat_to(o)), device_id_type=MESH)

    def a1(h, k):
        return rc(stA.at[h, k, pc], rxA.at[h, k], a1s.at[h, k], a1r.at[h, k], partner)

    def a2(h, k, o):
        return rc(
            sA.at[h, k, (z + o) % Z], rA.at[h, k, o], a2s.at[h, k, o], a2r.at[h, k, o], zdev(o)
        )

    def own_z(ref, ssem, rsem):
        def send(h, k, o):
            block = ref.at[h, k, c, z]
            return rc(block, block, ssem.at[h, k, o], rsem.at[h, k, o], zdev(o))

        def arrive(h, k, o):
            block = ref.at[h, k, c, (z + Z - o) % Z]
            return rc(block, block, ssem.at[h, k, o], rsem.at[h, k, o], zdev(o))

        return send, arrive

    def own_core(ref, ssem, rsem):
        def send(h, k):
            block = ref.at[h, k, c]
            return rc(block, block, ssem.at[h, k], rsem.at[h, k], partner)

        def arrive(h, k):
            block = ref.at[h, k, pc]
            return rc(block, block, ssem.at[h, k], rsem.at[h, k], partner)

        return send, arrive

    a3, a3in = own_z(acts, a3s, a3r)
    a4, a4in = own_core(acts, a4s, a4r)
    d3, d3in = own_z(dp, d3s, d3r)
    d4, d4in = own_core(dp, d4s, d4r)

    def combine_a(h, k):
        a1(h, k).wait_recv()
        sA[h, k] = stA[h, k, c] + rxA[h, k]
        for o in range(1, Z):
            a2(h, k, o).start()

    c_res.wait()
    pl.semaphore_wait(barrier, 1 + (Z - 1) + (NL - 1))

    def pre_part(h, k):
        p = jnp.dot(res_v[h * TH:(h + 1) * TH, :], enc_v[k], preferred_element_type=F32)
        for j in range(2):
            stA[h, k, j] = p[:, j * KC:(j + 1) * KC].reshape(Z, TB, KC)
        a1(h, k).start()

    def pre_first(k):
        enc_copy(k).wait()
        pre_part(0, k)

        @pl.when(k > 0)
        def _():
            combine_a(0, k - 1)

    loop(NK, pre_first)
    combine_a(0, NK - 1)
    for h in range(1, H):
        loop(NK, lambda k: pre_part(h, k))

    def fwd_a(h, k):
        for o in range(1, Z):
            a3in(h, k, o).wait_recv()
        a4(h, k).start()

    def act_step(h, k):
        for o in range(1, Z):
            a2(h, k, o).wait_recv()
        pre = sA[h, k, z]
        for o in range(1, Z):
            pre = pre + rA[h, k, o]
        pre = pre + bias[k, c]
        preS[h, k] = pre
        acts[h, k, c, z] = jnp.maximum(pre, 0.0).astype(BF16)
        for o in range(1, Z):
            a3(h, k, o).start()

    loop(NK, lambda k: act_step(0, k))
    loop(NK, lambda k: combine_a(1, k))

    def rt_step(n):
        rt_v[n] = res_v[:, pl.ds(pl.multiple_of(n * NB, NB), NB)].T

    loop(NN, rt_step)
    rt_copy = pltpu.make_async_copy(rt_v, rt_o, out_sem.at[0])
    rt_copy.start()

    def b1(h, n, o):
        to = lat_to(o)
        return rc(sB.at[h, n, to], rB.at[h, n, o], bs.at[h, n, o], br.at[h, n, o], (w, to))

    def c1(h, n, o):
        block = err.at[h, n, l]
        return rc(block, block, cs.at[h, n, o], cr.at[h, n, o], (w, lat_to(o)))

    def c1in(h, n, o):
        block = err.at[h, n, lat_from(o)]
        return rc(block, block, cs.at[h, n, o], cr.at[h, n, o], (w, lat_to(o)))

    def rec_step(h, n):
        a = jnp.concatenate(
            [acts[h, k, j].reshape(TH, KC) for k in range(NK) for j in range(2)], axis=1
        )
        r = jnp.dot(a, dec_v[n], preferred_element_type=F32).reshape(NL, TL, NB)
        rf[h, n] = r
        sB[h, n] = r.astype(BF16)
        for o in range(1, NL):
            b1(h, n, o).start()

    def at_step(h, k):
        a = jnp.concatenate([acts[h, k, j].reshape(TH, KC) for j in range(2)], axis=1)
        actsT[h, k] = a.T

    def err_step(h, n):
        for o in range(1, NL):
            b1(h, n, o).wait_recv()
        r = rf[h, n, l]
        for o in range(1, NL):
            r = r + rB[h, n, o].astype(F32)
        own = res_v[
            pl.ds(pl.multiple_of(h * TH + l * TL, TL), TL),
            pl.ds(pl.multiple_of(n * NB, NB), NB),
        ]
        err[h, n, l] = (r + dbias[n] - own.astype(F32)).astype(BF16)
        for o in range(1, NL):
            c1(h, n, o).start()

    def recon(h):
        loop(NK, lambda k: fwd_a(h, k))
        if h == 0:
            for n in range(NN):
                dec_copy(n).wait()
        loop(NK, lambda k: a4in(h, k).wait_recv())
        loop(NN, lambda n: rec_step(h, n))
        loop(NK, lambda k: at_step(h, k))

    recon(0)

    def zero_step(k):
        for s in range(3):
            sacc[s, k] = jnp.zeros(sacc.shape[2:], F32)

    loop(NK, zero_step)

    def err_act(i):
        err_step(0, i)
        act_step(1, i)

    loop(NK, err_act)
    recon(1)

    def dec_rows(n, k):
        return dec_v[n, pl.ds(pl.multiple_of(k * KB, KB), KB), :]

    def dacts_part(h, n, k):
        d = lax.dot_general(
            err[h, n].reshape(TH, NB), dec_rows(n, k), NT, preferred_element_type=F32
        )
        return [d[:, j * KC:(j + 1) * KC].reshape(Z, TB, KC) for j in range(2)]

    def grad_first(n, k):
        grad[n, k] = jnp.dot(
            actsT[0, k], err[0, n].reshape(TH, NB), preferred_element_type=F32
        )

    def grad_last(n, k):
        g = grad[n, k] + jnp.dot(
            actsT[1, k], err[1, n].reshape(TH, NB), preferred_element_type=F32
        )
        grad[n, k] = g
        wt = dec_rows(n, k).astype(F32)
        for s, prod in enumerate((wt * wt, g * wt, g * g)):
            part = prod[:, 0:128]
            for j in range(1, NB // 128):
                part = part + prod[:, j * 128:(j + 1) * 128]
            sacc[s, k] += part

    def err_wait(h, n):
        for o in range(1, NL):
            c1in(h, n, o).wait_recv()

    def d1(h, k):
        return rc(sD.at[h, k, pc], rxD.at[h, k], d1s.at[h, k], d1r.at[h, k], partner)

    def d2(h, k, o):
        return rc(
            sS.at[h, k, (z + o) % Z], rD.at[h, k, o], d2s.at[h, k, o], d2r.at[h, k, o], zdev(o)
        )

    def combine_d(h, k):
        d1(h, k).wait_recv()
        s = dacc[h, k, c] + rxD[h, k].astype(F32)
        dacc[h, k, c] = s
        sS[h, k] = s.astype(BF16)
        for o in range(1, Z):
            d2(h, k, o).start()

    def dacts_add(h, n, k):
        for j, d in enumerate(dacts_part(h, n, k)):
            if isinstance(n, int) and n == 0:
                dacc[h, k, j] = d
            else:
                dacc[h, k, j] += d

    last = NN - 1

    def d_step(h, k):
        for j, d in enumerate(dacts_part(h, last, k)):
            v = dacc[h, k, j] + d
            dacc[h, k, j] = v
            sD[h, k, j] = v.astype(BF16)
        d1(h, k).start()

        @pl.when(k > 0)
        def _():
            combine_d(h, k - 1)

    def dacts(h, beside):
        def step(n):
            err_wait(h, n)

            def k_step(k):
                dacts_add(h, n, k)
                beside(n, k)

            loop(NK, k_step)

        step(0)
        lax.fori_loop(1, last, lambda n, _: (step(n), 0)[1], 0)
        err_wait(h, last)
        loop(NK, lambda k: d_step(h, k))
        combine_d(h, NK - 1)

    def dp_step(h, k):
        for o in range(1, Z):
            d2(h, k, o).wait_recv()
        v = dacc[h, k, c, z]
        for o in range(1, Z):
            v = v + rD[h, k, o].astype(F32)
        dp[h, k, c, z] = jnp.where(preS[h, k] > 0.0, v + PENALTY, 0.0).astype(BF16)
        for o in range(1, Z):
            d3(h, k, o).start()

    def fwd_d(h, k):
        for o in range(1, Z):
            d3in(h, k, o).wait_recv()
        d4(h, k).start()

    dacts(0, lambda n, k: None)

    def err_grad(i):
        err_step(1, i)
        loop(NK, lambda k: grad_first(i, k))

    loop(NN, err_grad)
    loop(NK, lambda k: dp_step(0, k))
    dacts(1, grad_last)

    def gd_step(k):
        grad_last(last, k)
        for s in range(3):
            stv[k, s:s + 1, :] = jnp.sum(sacc[s, k].T, axis=0, keepdims=True)
        stv[k, 3:8, :] = jnp.zeros((5, KB), F32)
        dp_step(1, k)

    loop(NK, gd_step)

    e1 = rc(stv, rst, e1s, e1r, partner)
    e1.start()

    def e2(o):
        return rc(ss, rs2.at[o], e2s.at[o], e2r.at[o], zdev(o))

    loop(NK, lambda k: fwd_d(0, k))
    e1.wait_recv()
    ss[...] = stv[...] + rst[...]
    for o in range(1, Z):
        e2(o).start()

    loop(NK, lambda k: fwd_d(1, k))
    for o in range(1, Z):
        e2(o).wait_recv()

    def nd_copy(k):
        return pltpu.make_async_copy(
            nd_v.at[k], nd_o.at[pl.ds(pl.multiple_of(k * KB, KB), KB), :], out_sem.at[2 + k]
        )

    def nd_step(k):
        t = ss[k]
        for o in range(1, Z):
            t = t + rs2[o, k]
        ww, gw, gg = t[0:1], t[1:2], t[2:3]
        coef = gw / (ww + EPS)
        sq = (
            ww
            - 2.0 * STEP * (gw - coef * ww)
            + STEP * STEP * (gg - 2.0 * coef * gw + coef * coef * ww)
        )
        inv = 1.0 / jnp.sqrt(sq + EPS)
        up = jnp.broadcast_to((1.0 + STEP * coef) * inv, (128, KB)).T
        down = jnp.broadcast_to(STEP * inv, (128, KB)).T
        for n in range(NN):
            for j in range(NB // 128):
                wt = dec_v[n, pl.ds(pl.multiple_of(k * KB, KB), KB), j * 128:(j + 1) * 128]
                g = grad[n, k, :, j * 128:(j + 1) * 128]
                first = n * NB + j * 128
                nd_v[k, :, first:first + 128] = (wt.astype(F32) * up - g * down).astype(BF16)
        nd_copy(k).start()

    loop(NK, nd_step)
    for h in range(H):
        loop(NK, lambda k: d4in(h, k).wait_recv())
    dp_copy = pltpu.make_async_copy(dp, dp_o, out_sem.at[1])
    dp_copy.start()

    def drain(k):
        for h in range(H):
            for first in (a1, a4, d1, d4):
                first(h, k).wait_send()
            for o in range(1, Z):
                for each in (a2, a3, d2, d3):
                    each(h, k, o).wait_send()
        nd_copy(k).wait()

    def drain_n(n):
        for h in range(H):
            for o in range(1, NL):
                b1(h, n, o).wait_send()
                c1(h, n, o).wait_send()

    loop(NK, drain)
    loop(NN, drain_n)
    e1.wait_send()
    for o in range(1, Z):
        e2(o).wait_send()
    rt_copy.wait()
    dp_copy.wait()


def enc_grad_kernel(rt, dp, out):
    halves, blocks = dp.shape[:2]
    d = jnp.concatenate(
        [
            jnp.concatenate([dp[h, k] for k in range(blocks)], axis=1)
            for h in range(halves)
        ],
        axis=0,
    )
    out[...] = jnp.dot(rt[0], d, preferred_element_type=F32).astype(BF16)


def fused(W, NL, residuals, encoder, enc_bias, decoder, dec_bias):
    T, DW = residuals.shape
    LL = encoder.shape[1]
    Z = W // 2
    NK, NN = 4, 4
    KB, NB = LL // NK, DW // NN
    H = 2
    TH = T // H
    TB, TL = TH // Z, TH // NL
    KC = KB // 2
    V = pltpu.VMEM
    dma = pltpu.SemaphoreType.DMA
    sums, part, rows = (H, NK, 2, Z, TB, KC), (H, NK, Z, TB, KC), (H, NN, NL, TL, NB)
    one, per_z, per_l = (H, NK), (H, NK, Z), (H, NN, NL)
    scratch = [
        V((T, DW), BF16), V((NK, DW, KB), BF16), V((NN, LL, NB), BF16),
        V(sums, F32), V(part, F32), V(part, F32), V(part, F32), V((H, NK, TB, KC), F32),
        V(sums, BF16), V((H, NK, KB, TH), BF16), V((NN, NB, T), BF16),
        V(rows, F32), V(rows, BF16), V(rows, BF16), V(rows, BF16),
        V(sums, F32), V(sums, BF16), V(part, BF16), V(part, BF16), V(part, BF16), V(sums, BF16),
        V((NN, NK, KB, NB), F32), V((3, NK, KB, 128), F32),
        V((NK, 8, KB), F32), V((NK, 8, KB), F32), V((NK, 8, KB), F32), V((Z, NK, 8, KB), F32),
        V((NK, KB, DW), BF16),
        dma((1 + NK + NN,)), dma((2 + NK,)),
        dma(one), dma(one), dma(per_z), dma(per_z), dma(per_z), dma(per_z), dma(one), dma(one),
        dma(per_l), dma(per_l), dma(per_l), dma(per_l),
        dma(one), dma(one), dma(per_z), dma(per_z), dma(per_z), dma(per_z), dma(one), dma(one),
        dma, dma, dma((Z,)), dma((Z,)),
    ]
    hbm = pl.BlockSpec(memory_space=pl.ANY)
    vm = pl.BlockSpec(memory_space=pltpu.VMEM)
    new_decoder, dp, rt = pl.pallas_call(
        functools.partial(step_kernel, Z, NL, NK, NN),
        out_shape=(
            jax.ShapeDtypeStruct((LL, DW), BF16),
            jax.ShapeDtypeStruct(sums, BF16),
            jax.ShapeDtypeStruct((NN, NB, T), BF16),
        ),
        in_specs=[hbm, hbm, vm, hbm, vm],
        out_specs=(hbm, hbm, hbm),
        scratch_shapes=scratch,
        compiler_params=pltpu.CompilerParams(
            collective_id=0, has_side_effects=True, vmem_limit_bytes=60 * 2**20
        ),
        name="sae_step",
    )(residuals, encoder, enc_bias.reshape(NK, 2, 1, KC), decoder, dec_bias.reshape(NN, 1, NB))
    enc_grad = pl.pallas_call(
        enc_grad_kernel,
        grid=(NN,),
        out_shape=jax.ShapeDtypeStruct((DW, LL), BF16),
        in_specs=[
            pl.BlockSpec((1, NB, T), lambda i: (i, 0, 0)),
            pl.BlockSpec((H, 2 * NK, TH, KC), lambda i: (0, 0, 0, 0)),
        ],
        out_specs=pl.BlockSpec((NB, LL), lambda i: (i, 0)),
        compiler_params=pltpu.CompilerParams(vmem_limit_bytes=60 * 2**20),
        cost_estimate=pl.CostEstimate(
            flops=2 * T * DW * LL, bytes_accessed=2 * (T * DW + T * LL + DW * LL),
            transcendentals=0,
        ),
        name="enc_grad",
    )(rt, dp.reshape(H, 2 * NK, TH, KC))
    return enc_grad, new_decoder


def plain(residuals, encoder, enc_bias, decoder, dec_bias):
    tokens = residuals.shape[0]
    lat_count = lax.axis_size("lat")
    lat_rows = tokens // lat_count
    rows = residuals
    pre_rows = (
        lax.psum_scatter(
            jnp.dot(rows, encoder, preferred_element_type=jnp.float32),
            "width",
            scatter_dimension=0,
            tiled=True,
        )
        + enc_bias
    )
    active_rows = pre_rows > 0.0
    act_rows = jnp.maximum(pre_rows, 0.0).astype(jnp.bfloat16)
    acts = lax.all_gather(act_rows, "width", axis=0, tiled=True)
    rows = acts
    recon_rows = lax.psum_scatter(
        jnp.dot(rows, decoder, preferred_element_type=jnp.float32),
        "lat",
        scatter_dimension=0,
        tiled=True,
    )
    first = lax.axis_index("lat") * lat_rows
    own_rows = lax.dynamic_slice_in_dim(residuals, first, lat_rows, 0)
    error_part = (recon_rows + dec_bias - own_rows.astype(jnp.float32)).astype(jnp.bfloat16)
    error = lax.all_gather(error_part, "lat", axis=0, tiled=True)
    rows = error
    dacts_rows = (
        lax.psum_scatter(
            lax.dot_general(
                rows, decoder, (((1,), (1,)), ((), ())), preferred_element_type=jnp.float32
            ),
            "width",
            scatter_dimension=0,
            tiled=True,
        )
        + PENALTY
    )
    dpre_part = jnp.where(active_rows, dacts_rows, 0.0).astype(jnp.bfloat16)
    dpre = lax.all_gather(dpre_part, "width", axis=0, tiled=True)
    enc_grad = lax.dot_general(
        residuals, dpre, (((0,), (0,)), ((), ())), preferred_element_type=jnp.float32
    ).astype(jnp.bfloat16)
    grad = lax.dot_general(
        acts, error, (((0,), (0,)), ((), ())), preferred_element_type=jnp.float32
    )
    weight = decoder.astype(jnp.float32)
    ww, gw, gg = lax.psum(
        (
            jnp.sum(weight * weight, axis=1),
            jnp.sum(grad * weight, axis=1),
            jnp.sum(grad * grad, axis=1),
        ),
        "width",
    )
    coef_row = gw / (ww + EPS)
    coef = coef_row[:, None]
    moved = weight - STEP * (grad - coef * weight)
    squared = (
        ww
        - 2.0 * STEP * (gw - coef_row * ww)
        + STEP * STEP * (gg - 2.0 * coef_row * gw + coef_row * coef_row * ww)
    )
    new_decoder = (moved / jnp.sqrt(squared + EPS)[:, None]).astype(jnp.bfloat16)
    return (enc_grad, new_decoder)


def per_device(W, NL, residuals, encoder, enc_bias, decoder, dec_bias):
    T, DW = residuals.shape
    LL = encoder.shape[1]
    args = (residuals, encoder, enc_bias, decoder, dec_bias)
    fits = W % 2 == 0 and NL % 2 == 0 and T % (16 * W) == 0 and T % (32 * NL) == 0
    if fits and DW % 512 == 0 and LL % 1024 == 0 and T % 128 == 0:
        return fused(W, NL, *args)
    return plain(*args)


def solution(mesh):
    return jax.shard_map(
        functools.partial(per_device, mesh.shape["width"], mesh.shape["lat"]),
        mesh=mesh,
        in_specs=(P(None, "width"), P("width", "lat"), P("lat"), P("lat", "width"), P("width")),
        out_specs=(P("width", "lat"), P("lat", "width")),
        check_vma=False,
    )
```

```python
import functools

import jax
import jax.numpy as jnp
from jax import lax
from jax.experimental import pallas as pl
from jax.experimental.pallas import tpu as pltpu
from jax.sharding import PartitionSpec as P

EPS = 1e-06
STEP = 0.0003
PENALTY = 0.5
MESH = pl.DeviceIdType.MESH
F32, BF16 = jnp.float32, jnp.bfloat16
NT = (((1,), (1,)), ((), ()))


def step_kernel(
    Z, NL, NK, NN,
    res_h, enc_h, bias, dec_h, dbias,
    nd_o, dp_o, rt_o,
    res_v, enc_v, dec_v, stA, rxA, sA, rA, preS, acts, actsT, rt_v,
    rf, sB, sB2, rB, err, dacc, sD, rxD, sS, rD, dp, grad, sacc, stv, rst, ss, rs2, nd_v,
    in_sem, out_sem,
    a1s, a1r, a2s, a2r, a3s, a3r, a4s, a4r,
    bs, br, cs, cr,
    d1s, d1r, d2s, d2r, d3s, d3r, d4s, d4r,
    e1s, e1r, e2s, e2r,
):
    T, DW = res_v.shape
    H = acts.shape[0]
    TH = T // H
    TB, KC = acts.shape[-2:]
    KB = 2 * KC
    TL, NB = err.shape[-2:]
    w = lax.axis_index("width")
    l = lax.axis_index("lat")
    z, c = w // 2, w % 2
    pc = 1 - c
    partner = (z * 2 + pc, l)

    def zdev(o):
        return ((z + o) % Z) * 2 + c, l

    def lat_to(o):
        return ((l // 2 + o // 2) % (NL // 2)) * 2 + (l % 2 + o % 2) % 2

    ly, lx = l // 2, l % 2
    diag = (1 - ly) * 2 + 1 - lx

    def first_of(n):
        q = (n + c) % 2
        return (ly + q) % 2 * 2 + (lx + 1 - q) % 2

    def second_of(n):
        q = (n + c) % 2
        return (ly + 1 - q) % 2 * 2 + (lx + q) % 2

    def rc(src, dst, ssem, rsem, dev):
        return pltpu.make_async_remote_copy(
            src_ref=src, dst_ref=dst, send_sem=ssem, recv_sem=rsem,
            device_id=dev, device_id_type=MESH,
        )

    def loop(n, f):
        lax.fori_loop(0, n, lambda i, _: (f(i), 0)[1], 0)

    c_res = pltpu.make_async_copy(res_h, res_v, in_sem.at[0])
    c_res.start()

    def enc_copy(k):
        return pltpu.make_async_copy(
            enc_h.at[:, pl.ds(pl.multiple_of(k * KB, KB), KB)], enc_v.at[k], in_sem.at[1 + k]
        )

    def dec_copy(n):
        return pltpu.make_async_copy(
            dec_h.at[:, pl.ds(pl.multiple_of(n * NB, NB), NB)], dec_v.at[n], in_sem.at[1 + NK + n]
        )

    for k in range(NK):
        enc_copy(k).start()
    for n in range(NN):
        dec_copy(n).start()

    barrier = pltpu.get_barrier_semaphore()
    pl.semaphore_signal(barrier, inc=1, device_id=partner, device_id_type=MESH)
    for o in range(1, Z):
        pl.semaphore_signal(barrier, inc=1, device_id=zdev(o), device_id_type=MESH)
    for o in range(1, NL):
        pl.semaphore_signal(barrier, inc=1, device_id=(w, lat_to(o)), device_id_type=MESH)

    def a1(h, k):
        return rc(stA.at[h, k, pc], rxA.at[h, k], a1s.at[h, k], a1r.at[h, k], partner)

    def a2(h, k, o):
        return rc(
            sA.at[h, k, (z + o) % Z], rA.at[h, k, o], a2s.at[h, k, o], a2r.at[h, k, o], zdev(o)
        )

    def own_z(ref, ssem, rsem):
        def send(h, k, o):
            block = ref.at[h, k, c, z]
            return rc(block, block, ssem.at[h, k, o], rsem.at[h, k, o], zdev(o))

        def arrive(h, k, o):
            block = ref.at[h, k, c, (z + Z - o) % Z]
            return rc(block, block, ssem.at[h, k, o], rsem.at[h, k, o], zdev(o))

        return send, arrive

    def own_core(ref, ssem, rsem):
        def send(h, k):
            block = ref.at[h, k, c]
            return rc(block, block, ssem.at[h, k], rsem.at[h, k], partner)

        def arrive(h, k):
            block = ref.at[h, k, pc]
            return rc(block, block, ssem.at[h, k], rsem.at[h, k], partner)

        return send, arrive

    a3, a3in = own_z(acts, a3s, a3r)
    a4, a4in = own_core(acts, a4s, a4r)
    d3, d3in = own_z(dp, d3s, d3r)
    d4, d4in = own_core(dp, d4s, d4r)

    def combine_a(h, k):
        a1(h, k).wait_recv()
        sA[h, k] = stA[h, k, c] + rxA[h, k]
        for o in range(1, Z):
            a2(h, k, o).start()

    c_res.wait()
    pl.semaphore_wait(barrier, 1 + (Z - 1) + (NL - 1))

    def pre_part(h, k):
        p = jnp.dot(res_v[h * TH:(h + 1) * TH, :], enc_v[k], preferred_element_type=F32)
        for j in range(2):
            stA[h, k, j] = p[:, j * KC:(j + 1) * KC].reshape(Z, TB, KC)
        a1(h, k).start()

    def pre_first(k):
        enc_copy(k).wait()
        pre_part(0, k)

        @pl.when(k > 0)
        def _():
            combine_a(0, k - 1)

    loop(NK, pre_first)
    combine_a(0, NK - 1)
    for h in range(1, H):
        loop(NK, lambda k: pre_part(h, k))

    def fwd_a(h, k):
        for o in range(1, Z):
            a3in(h, k, o).wait_recv()
        a4(h, k).start()

    def act_step(h, k):
        for o in range(1, Z):
            a2(h, k, o).wait_recv()
        pre = sA[h, k, z]
        for o in range(1, Z):
            pre = pre + rA[h, k, o]
        pre = pre + bias[k, c]
        preS[h, k] = pre
        acts[h, k, c, z] = jnp.maximum(pre, 0.0).astype(BF16)
        for o in range(1, Z):
            a3(h, k, o).start()

    loop(NK, lambda k: act_step(0, k))
    loop(NK, lambda k: combine_a(1, k))

    def rt_step(n):
        rt_v[n] = res_v[:, pl.ds(pl.multiple_of(n * NB, NB), NB)].T

    loop(NN, rt_step)
    rt_copy = pltpu.make_async_copy(rt_v, rt_o, out_sem.at[0])
    rt_copy.start()

    def b1(h, n, o):
        to = first_of(n)
        return rc(
            sB.at[h, n, to if o == 0 else diag], rB.at[h, n, o],
            bs.at[h, n, o], br.at[h, n, o], (w, to),
        )

    def b2(h, n):
        return rc(
            sB2.at[h, n], rB.at[h, n, 2], bs.at[h, n, 2], br.at[h, n, 2], (w, second_of(n))
        )

    def c_copy(h, n, o, block, to):
        ref = err.at[h, n, block]
        return rc(ref, ref, cs.at[h, n, o], cr.at[h, n, o], (w, to))

    def c1(h, n):
        return c_copy(h, n, 0, l, second_of(n))

    def c1in(h, n):
        return c_copy(h, n, 0, second_of(n), second_of(n))

    def c2(h, n):
        return c_copy(h, n, 1, l, first_of(n))

    def c2in(h, n):
        return c_copy(h, n, 1, first_of(n), first_of(n))

    def c3(h, n):
        return c_copy(h, n, 2, second_of(n), first_of(n))

    def c3in(h, n):
        return c_copy(h, n, 2, diag, first_of(n))

    def rec_step(h, n):
        a = jnp.concatenate(
            [acts[h, k, j].reshape(TH, KC) for k in range(NK) for j in range(2)], axis=1
        )
        r = jnp.dot(a, dec_v[n], preferred_element_type=F32).reshape(NL, TL, NB)
        rf[h, n] = r
        sB[h, n] = r.astype(BF16)
        b1(h, n, 1).start()
        b1(h, n, 0).start()

    def mid_step(h, n):
        b1(h, n, 1).wait_recv()
        sB2[h, n] = (rf[h, n, second_of(n)] + rB[h, n, 1].astype(F32)).astype(BF16)
        b2(h, n).start()

    def at_step(h, k):
        a = jnp.concatenate([acts[h, k, j].reshape(TH, KC) for j in range(2)], axis=1)
        actsT[h, k] = a.T

    def err_step(h, n):
        b1(h, n, 0).wait_recv()
        b2(h, n).wait_recv()
        r = rf[h, n, l] + rB[h, n, 0].astype(F32) + rB[h, n, 2].astype(F32)
        own = res_v[
            pl.ds(pl.multiple_of(h * TH + l * TL, TL), TL),
            pl.ds(pl.multiple_of(n * NB, NB), NB),
        ]
        err[h, n, l] = (r + dbias[n] - own.astype(F32)).astype(BF16)
        c1(h, n).start()
        c2(h, n).start()

    def fwd_err(h, n):
        c1in(h, n).wait_recv()
        c3(h, n).start()

    def recon(h):
        loop(NK, lambda k: fwd_a(h, k))
        if h == 0:
            for n in range(NN):
                dec_copy(n).wait()
        loop(NK, lambda k: a4in(h, k).wait_recv())
        loop(NN, lambda n: rec_step(h, n))
        loop(NK, lambda k: at_step(h, k))

    recon(0)

    def zero_step(k):
        for s in range(3):
            sacc[s, k] = jnp.zeros(sacc.shape[2:], F32)

    loop(NK, zero_step)

    loop(NN, lambda n: mid_step(0, n))

    def err_act(i):
        err_step(0, i)
        act_step(1, i)

        @pl.when(i > 0)
        def _():
            fwd_err(0, i - 1)

    loop(NK, err_act)
    fwd_err(0, NN - 1)
    recon(1)

    def dec_rows(n, k):
        return dec_v[n, pl.ds(pl.multiple_of(k * KB, KB), KB), :]

    def dacts_part(h, n, k):
        d = lax.dot_general(
            err[h, n].reshape(TH, NB), dec_rows(n, k), NT, preferred_element_type=F32
        )
        return [d[:, j * KC:(j + 1) * KC].reshape(Z, TB, KC) for j in range(2)]

    def grad_first(n, k):
        grad[n, k] = jnp.dot(
            actsT[0, k], err[0, n].reshape(TH, NB), preferred_element_type=F32
        )

    def grad_last(n, k):
        g = grad[n, k] + jnp.dot(
            actsT[1, k], err[1, n].reshape(TH, NB), preferred_element_type=F32
        )
        grad[n, k] = g
        wt = dec_rows(n, k).astype(F32)
        for s, prod in enumerate((wt * wt, g * wt, g * g)):
            part = prod[:, 0:128]
            for j in range(1, NB // 128):
                part = part + prod[:, j * 128:(j + 1) * 128]
            sacc[s, k] += part

    def err_wait(h, n):
        c2in(h, n).wait_recv()
        c3in(h, n).wait_recv()

    def d1(h, k):
        return rc(sD.at[h, k, pc], rxD.at[h, k], d1s.at[h, k], d1r.at[h, k], partner)

    def d2(h, k, o):
        return rc(
            sS.at[h, k, (z + o) % Z], rD.at[h, k, o], d2s.at[h, k, o], d2r.at[h, k, o], zdev(o)
        )

    def combine_d(h, k):
        d1(h, k).wait_recv()
        s = dacc[h, k, c] + rxD[h, k].astype(F32)
        dacc[h, k, c] = s
        sS[h, k] = s.astype(BF16)
        for o in range(1, Z):
            d2(h, k, o).start()

    def dacts_add(h, n, k):
        for j, d in enumerate(dacts_part(h, n, k)):
            if isinstance(n, int) and n == 0:
                dacc[h, k, j] = d
            else:
                dacc[h, k, j] += d

    last = NN - 1

    def d_step(h, k):
        for j, d in enumerate(dacts_part(h, last, k)):
            v = dacc[h, k, j] + d
            dacc[h, k, j] = v
            sD[h, k, j] = v.astype(BF16)
        d1(h, k).start()

        @pl.when(k > 0)
        def _():
            combine_d(h, k - 1)

    def dacts(h, beside, after):
        def step(n):
            err_wait(h, n)

            def k_step(k):
                dacts_add(h, n, k)
                beside(n, k)

            loop(NK, k_step)
            after(n)

        step(0)
        lax.fori_loop(1, last, lambda n, _: (step(n), 0)[1], 0)
        err_wait(h, last)
        loop(NK, lambda k: d_step(h, k))
        combine_d(h, NK - 1)
        after(last)

    def dp_step(h, k):
        for o in range(1, Z):
            d2(h, k, o).wait_recv()
        v = dacc[h, k, c, z]
        for o in range(1, Z):
            v = v + rD[h, k, o].astype(F32)
        dp[h, k, c, z] = jnp.where(preS[h, k] > 0.0, v + PENALTY, 0.0).astype(BF16)
        for o in range(1, Z):
            d3(h, k, o).start()

    def fwd_d(h, k):
        for o in range(1, Z):
            d3in(h, k, o).wait_recv()
        d4(h, k).start()

    dacts(0, lambda n, k: None, lambda n: mid_step(1, n))

    def err_grad(i):
        err_step(1, i)
        loop(NK, lambda k: grad_first(i, k))

        @pl.when(i > 0)
        def _():
            fwd_err(1, i - 1)

    loop(NN, err_grad)
    fwd_err(1, NN - 1)
    loop(NK, lambda k: dp_step(0, k))
    dacts(1, grad_last, lambda n: None)

    def gd_step(k):
        grad_last(last, k)
        for s in range(3):
            stv[k, s:s + 1, :] = jnp.sum(sacc[s, k].T, axis=0, keepdims=True)
        stv[k, 3:8, :] = jnp.zeros((5, KB), F32)
        dp_step(1, k)

    loop(NK, gd_step)

    e1 = rc(stv, rst, e1s, e1r, partner)
    e1.start()

    def e2(o):
        return rc(ss, rs2.at[o], e2s.at[o], e2r.at[o], zdev(o))

    loop(NK, lambda k: fwd_d(0, k))
    e1.wait_recv()
    ss[...] = stv[...] + rst[...]
    for o in range(1, Z):
        e2(o).start()

    loop(NK, lambda k: fwd_d(1, k))
    for o in range(1, Z):
        e2(o).wait_recv()

    def nd_copy(k):
        return pltpu.make_async_copy(
            nd_v.at[k], nd_o.at[pl.ds(pl.multiple_of(k * KB, KB), KB), :], out_sem.at[2 + k]
        )

    def nd_step(k):
        t = ss[k]
        for o in range(1, Z):
            t = t + rs2[o, k]
        ww, gw, gg = t[0:1], t[1:2], t[2:3]
        coef = gw / (ww + EPS)
        sq = (
            ww
            - 2.0 * STEP * (gw - coef * ww)
            + STEP * STEP * (gg - 2.0 * coef * gw + coef * coef * ww)
        )
        inv = 1.0 / jnp.sqrt(sq + EPS)
        up = jnp.broadcast_to((1.0 + STEP * coef) * inv, (128, KB)).T
        down = jnp.broadcast_to(STEP * inv, (128, KB)).T
        for n in range(NN):
            for j in range(NB // 128):
                wt = dec_v[n, pl.ds(pl.multiple_of(k * KB, KB), KB), j * 128:(j + 1) * 128]
                g = grad[n, k, :, j * 128:(j + 1) * 128]
                first = n * NB + j * 128
                nd_v[k, :, first:first + 128] = (wt.astype(F32) * up - g * down).astype(BF16)
        nd_copy(k).start()

    loop(NK, nd_step)
    for h in range(H):
        loop(NK, lambda k: d4in(h, k).wait_recv())
    dp_copy = pltpu.make_async_copy(dp, dp_o, out_sem.at[1])
    dp_copy.start()

    def drain(k):
        for h in range(H):
            for first in (a1, a4, d1, d4):
                first(h, k).wait_send()
            for o in range(1, Z):
                for each in (a2, a3, d2, d3):
                    each(h, k, o).wait_send()
        nd_copy(k).wait()

    def drain_n(n):
        for h in range(H):
            for o in range(2):
                b1(h, n, o).wait_send()
            for each in (b2, c1, c2, c3):
                each(h, n).wait_send()

    loop(NK, drain)
    loop(NN, drain_n)
    e1.wait_send()
    for o in range(1, Z):
        e2(o).wait_send()
    rt_copy.wait()
    dp_copy.wait()


def enc_grad_kernel(rt, dp, nd, out, nd_out):
    nd_out[...] = nd[...]
    halves, blocks = dp.shape[:2]
    d = jnp.concatenate(
        [
            jnp.concatenate([dp[h, k] for k in range(blocks)], axis=1)
            for h in range(halves)
        ],
        axis=0,
    )
    out[...] = jnp.dot(rt[0], d, preferred_element_type=F32).astype(BF16)


def fused(W, NL, residuals, encoder, enc_bias, decoder, dec_bias):
    T, DW = residuals.shape
    LL = encoder.shape[1]
    Z = W // 2
    NK, NN = 4, 4
    KB, NB = LL // NK, DW // NN
    H = 2
    TH = T // H
    TB, TL = TH // Z, TH // NL
    KC = KB // 2
    V = pltpu.VMEM
    dma = pltpu.SemaphoreType.DMA
    sums, part, rows = (H, NK, 2, Z, TB, KC), (H, NK, Z, TB, KC), (H, NN, NL, TL, NB)
    one, per_z, per_l = (H, NK), (H, NK, Z), (H, NN, 3)
    scratch = [
        V((T, DW), BF16), V((NK, DW, KB), BF16), V((NN, LL, NB), BF16),
        V(sums, F32), V(part, F32), V(part, F32), V(part, F32), V((H, NK, TB, KC), F32),
        V(sums, BF16), V((H, NK, KB, TH), BF16), V((NN, NB, T), BF16),
        V(rows, F32), V(rows, BF16), V((H, NN, TL, NB), BF16), V((H, NN, 3, TL, NB), BF16), V(rows, BF16),
        V(sums, F32), V(sums, BF16), V(part, BF16), V(part, BF16), V(part, BF16), V(sums, BF16),
        V((NN, NK, KB, NB), F32), V((3, NK, KB, 128), F32),
        V((NK, 8, KB), F32), V((NK, 8, KB), F32), V((NK, 8, KB), F32), V((Z, NK, 8, KB), F32),
        V((NK, KB, DW), BF16),
        dma((1 + NK + NN,)), dma((2 + NK,)),
        dma(one), dma(one), dma(per_z), dma(per_z), dma(per_z), dma(per_z), dma(one), dma(one),
        dma(per_l), dma(per_l), dma(per_l), dma(per_l),
        dma(one), dma(one), dma(per_z), dma(per_z), dma(per_z), dma(per_z), dma(one), dma(one),
        dma, dma, dma((Z,)), dma((Z,)),
    ]
    hbm = pl.BlockSpec(memory_space=pl.ANY)
    vm = pl.BlockSpec(memory_space=pltpu.VMEM)
    new_decoder, dp, rt = pl.pallas_call(
        functools.partial(step_kernel, Z, NL, NK, NN),
        out_shape=(
            jax.ShapeDtypeStruct((LL, DW), BF16),
            jax.ShapeDtypeStruct(sums, BF16),
            jax.ShapeDtypeStruct((NN, NB, T), BF16),
        ),
        in_specs=[hbm, hbm, vm, hbm, vm],
        out_specs=(hbm, hbm, hbm),
        scratch_shapes=scratch,
        compiler_params=pltpu.CompilerParams(
            collective_id=0, has_side_effects=True, vmem_limit_bytes=60 * 2**20
        ),
        name="sae_step",
    )(residuals, encoder, enc_bias.reshape(NK, 2, 1, KC), decoder, dec_bias.reshape(NN, 1, NB))
    enc_grad, new_decoder = pl.pallas_call(
        enc_grad_kernel,
        grid=(2 * NN,),
        out_shape=(
            jax.ShapeDtypeStruct((DW, LL), BF16),
            jax.ShapeDtypeStruct((LL, DW), BF16),
        ),
        in_specs=[
            pl.BlockSpec((1, NB // 2, T), lambda i: (i // 2, i % 2, 0)),
            pl.BlockSpec((H, 2 * NK, TH, KC), lambda i: (0, 0, 0, 0)),
            pl.BlockSpec((LL // (2 * NN), DW), lambda i: (i, 0)),
        ],
        out_specs=(
            pl.BlockSpec((NB // 2, LL), lambda i: (i, 0)),
            pl.BlockSpec((LL // (2 * NN), DW), lambda i: (i, 0)),
        ),
        compiler_params=pltpu.CompilerParams(vmem_limit_bytes=60 * 2**20),
        cost_estimate=pl.CostEstimate(
            flops=2 * T * DW * LL, bytes_accessed=2 * (T * DW + T * LL + 3 * DW * LL),
            transcendentals=0,
        ),
        name="enc_grad",
    )(rt, dp.reshape(H, 2 * NK, TH, KC), new_decoder)
    return enc_grad, new_decoder


def plain(residuals, encoder, enc_bias, decoder, dec_bias):
    tokens = residuals.shape[0]
    lat_count = lax.axis_size("lat")
    lat_rows = tokens // lat_count
    rows = residuals
    pre_rows = (
        lax.psum_scatter(
            jnp.dot(rows, encoder, preferred_element_type=jnp.float32),
            "width",
            scatter_dimension=0,
            tiled=True,
        )
        + enc_bias
    )
    active_rows = pre_rows > 0.0
    act_rows = jnp.maximum(pre_rows, 0.0).astype(jnp.bfloat16)
    acts = lax.all_gather(act_rows, "width", axis=0, tiled=True)
    rows = acts
    recon_rows = lax.psum_scatter(
        jnp.dot(rows, decoder, preferred_element_type=jnp.float32),
        "lat",
        scatter_dimension=0,
        tiled=True,
    )
    first = lax.axis_index("lat") * lat_rows
    own_rows = lax.dynamic_slice_in_dim(residuals, first, lat_rows, 0)
    error_part = (recon_rows + dec_bias - own_rows.astype(jnp.float32)).astype(jnp.bfloat16)
    error = lax.all_gather(error_part, "lat", axis=0, tiled=True)
    rows = error
    dacts_rows = (
        lax.psum_scatter(
            lax.dot_general(
                rows, decoder, (((1,), (1,)), ((), ())), preferred_element_type=jnp.float32
            ),
            "width",
            scatter_dimension=0,
            tiled=True,
        )
        + PENALTY
    )
    dpre_part = jnp.where(active_rows, dacts_rows, 0.0).astype(jnp.bfloat16)
    dpre = lax.all_gather(dpre_part, "width", axis=0, tiled=True)
    enc_grad = lax.dot_general(
        residuals, dpre, (((0,), (0,)), ((), ())), preferred_element_type=jnp.float32
    ).astype(jnp.bfloat16)
    grad = lax.dot_general(
        acts, error, (((0,), (0,)), ((), ())), preferred_element_type=jnp.float32
    )
    weight = decoder.astype(jnp.float32)
    ww, gw, gg = lax.psum(
        (
            jnp.sum(weight * weight, axis=1),
            jnp.sum(grad * weight, axis=1),
            jnp.sum(grad * grad, axis=1),
        ),
        "width",
    )
    coef_row = gw / (ww + EPS)
    coef = coef_row[:, None]
    moved = weight - STEP * (grad - coef * weight)
    squared = (
        ww
        - 2.0 * STEP * (gw - coef_row * ww)
        + STEP * STEP * (gg - 2.0 * coef_row * gw + coef_row * coef_row * ww)
    )
    new_decoder = (moved / jnp.sqrt(squared + EPS)[:, None]).astype(jnp.bfloat16)
    return (enc_grad, new_decoder)


def per_device(W, NL, residuals, encoder, enc_bias, decoder, dec_bias):
    T, DW = residuals.shape
    LL = encoder.shape[1]
    args = (residuals, encoder, enc_bias, decoder, dec_bias)
    fits = W % 2 == 0 and NL == 4 and T % (16 * W) == 0 and T % (32 * NL) == 0
    if fits and DW % 512 == 0 and LL % 1024 == 0 and T % 128 == 0:
        return fused(W, NL, *args)
    return plain(*args)


def solution(mesh):
    return jax.shard_map(
        functools.partial(per_device, mesh.shape["width"], mesh.shape["lat"]),
        mesh=mesh,
        in_specs=(P(None, "width"), P("width", "lat"), P("lat"), P("lat", "width"), P("width")),
        out_specs=(P("width", "lat"), P("lat", "width")),
        check_vma=False,
    )
```
